8 devices in a mesh: fsdp: 8 (over z, y, x, core).
Axes of the slice: x: 2, y: 2, z: 1, core: 2. Of those that a mesh axis runs over, the one named last changes fastest.
Arguments:
- features: bfloat16 [24, 64, 1536], P('fsdp')
- tokens: int32 [24, 64], P('fsdp')
- embedding: bfloat16 [151936, 1536], replicated
- lm_head: bfloat16 [151936, 1536], replicated
- w_fc: bfloat16 [3072, 1536], P('fsdp')
- b_fc: bfloat16 [1536], P('fsdp')
- w_q: bfloat16 [1536, 12, 128], P('fsdp')
- w_k: bfloat16 [1536, 2, 128], P('fsdp')
- w_v: bfloat16 [1536, 2, 128], P('fsdp')
- w_o: bfloat16 [1536, 1536], P('fsdp')
- g_norm: bfloat16 [1536], P('fsdp')
- w_gate: bfloat16 [1536, 8960], P('fsdp')
- w_up: bfloat16 [1536, 8960], P('fsdp')
- w_down: bfloat16 [8960, 1536], P('fsdp')
Outputs:
- output 1: float32 [], replicated
- output 2: float32 [3072, 1536], P('fsdp')
- output 3: float32 [1536], P('fsdp')
- output 4: float32 [1536, 12, 128], P('fsdp')
- output 5: float32 [1536, 2, 128], P('fsdp')
- output 6: float32 [1536, 2, 128], P('fsdp')
- output 7: float32 [1536, 1536], P('fsdp')
- output 8: float32 [1536], P('fsdp')
- output 9: float32 [1536, 8960], P('fsdp')
- output 10: float32 [1536, 8960], P('fsdp')
- output 11: float32 [8960, 1536], P('fsdp')
All inputs are finite; a program needn't handle non-finite values.
Results may differ from the reference program's by a relative error of at most 0.02.
Values are sent between devices in bfloat16 or wider.
A program may use at most 3.75 GiB of HBM per device.

```python
import math
import jax
import jax.numpy as jnp
from jax import lax

D = 1536
HEADS = 12
KV_HEADS = 2
HEAD = 128
FF = 8960
VOCAB = 151936
SEQ = 64
BATCH = 24
ROPE_BASE = 10000
NORM_EPS = 1e-5
CLS_WEIGHT = 0.1


def setup_inputs(seed: int = 0) -> dict:
    key_list = jax.random.split(jax.random.key(seed), 14)

    def gaussian(key_index, out_shape, spread):
        return jax.random.normal(key_list[key_index], out_shape, jnp.float32) * spread

    return {
        "features": gaussian(0, (BATCH, SEQ, D), 1.0).astype(jnp.bfloat16),
        "tokens": jax.random.randint(key_list[1], (BATCH, SEQ), 0, VOCAB, jnp.int32),
        "embedding": gaussian(2, (VOCAB, D), 1.0).astype(jnp.bfloat16),
        "lm_head": gaussian(3, (VOCAB, D), 2.0 / math.sqrt(D)).astype(jnp.bfloat16),
        "w_fc": gaussian(4, (2 * D, D), 1.0 / math.sqrt(2 * D)).astype(jnp.bfloat16),
        "b_fc": gaussian(5, (D,), 0.5).astype(jnp.bfloat16),
        "w_q": gaussian(6, (D, HEADS, HEAD), 1.0 / math.sqrt(D)).astype(jnp.bfloat16),
        "w_k": gaussian(7, (D, KV_HEADS, HEAD), 1.0 / math.sqrt(D)).astype(jnp.bfloat16),
        "w_v": gaussian(8, (D, KV_HEADS, HEAD), 1.0 / math.sqrt(D)).astype(jnp.bfloat16),
        "w_o": gaussian(9, (HEADS * HEAD, D), 1.0 / math.sqrt(HEADS * HEAD)).astype(jnp.bfloat16),
        "g_norm": (1.0 + gaussian(10, (D,), 0.3)).astype(jnp.bfloat16),
        "w_gate": gaussian(11, (D, FF), 1.0 / math.sqrt(D)).astype(jnp.bfloat16),
        "w_up": gaussian(12, (D, FF), 1.0 / math.sqrt(D)).astype(jnp.bfloat16),
        "w_down": gaussian(13, (FF, D), 1.0 / math.sqrt(FF)).astype(jnp.bfloat16),
    }


def rope_tables(seq_len, head_dim):
    half_dim = head_dim // 2
    inv_freq = jnp.exp(jnp.arange(half_dim, dtype=jnp.float32) * (-2.0 * math.log(ROPE_BASE) / head_dim))
    angles = jnp.arange(seq_len, dtype=jnp.float32)[:, None] * inv_freq[None, :]
    return jnp.cos(angles), jnp.sin(angles)


def apply_rope(projected, cos_tab, sin_tab):
    half_dim = projected.shape[-1] // 2
    first_half = projected[..., :half_dim]
    second_half = projected[..., half_dim:]
    cos_rows = cos_tab[:, None, :]
    sin_rows = sin_tab[:, None, :]
    return jnp.concatenate([first_half * cos_rows - second_half * sin_rows, second_half * cos_rows + first_half * sin_rows], axis=-1)


def draft_forward(weights, features, tokens, embedding):
    w_fc, b_fc, w_q, w_k, w_v, w_o, g_norm, w_gate, w_up, w_down = weights
    seq_len, model_width = features.shape
    head_count, head_dim = w_q.shape[1], w_q.shape[2]
    kv_count = w_k.shape[1]
    fused_in = jnp.concatenate([features, embedding[tokens]], axis=-1)
    hidden0 = (jnp.dot(fused_in, w_fc, preferred_element_type=jnp.float32) + b_fc.astype(jnp.float32)).astype(jnp.bfloat16)
    q_proj = jnp.dot(hidden0, w_q.reshape(model_width, head_count * head_dim), preferred_element_type=jnp.float32).reshape(seq_len, head_count, head_dim)
    k_proj = jnp.dot(hidden0, w_k.reshape(model_width, kv_count * head_dim), preferred_element_type=jnp.float32).reshape(seq_len, kv_count, head_dim)
    v_heads = jnp.dot(hidden0, w_v.reshape(model_width, kv_count * head_dim), preferred_element_type=jnp.float32).astype(jnp.bfloat16).reshape(seq_len, kv_count, head_dim)
    cos_tab, sin_tab = rope_tables(seq_len, head_dim)
    queries = apply_rope(q_proj, cos_tab, sin_tab).astype(jnp.bfloat16).reshape(seq_len, kv_count, head_count // kv_count, head_dim)
    keys_rot = apply_rope(k_proj, cos_tab, sin_tab).astype(jnp.bfloat16)
    scores = jnp.einsum("qkgd,skd->kgqs", queries.astype(jnp.float32), keys_rot.astype(jnp.float32)) * (1.0 / math.sqrt(head_dim))
    causal = jnp.arange(seq_len)[:, None] >= jnp.arange(seq_len)[None, :]
    attn_probs = jax.nn.softmax(jnp.where(causal, scores, -1e30), axis=-1).astype(jnp.bfloat16)
    attn_mixed = jnp.einsum("kgqs,skd->qkgd", attn_probs.astype(jnp.float32), v_heads.astype(jnp.float32)).astype(jnp.bfloat16).reshape(seq_len, head_count * head_dim)
    hidden1 = (hidden0.astype(jnp.float32) + jnp.dot(attn_mixed, w_o, preferred_element_type=jnp.float32)).astype(jnp.bfloat16)
    h1_f32 = hidden1.astype(jnp.float32)
    inv_rms = lax.rsqrt(jnp.mean(h1_f32 * h1_f32, axis=-1, keepdims=True) + NORM_EPS)
    normed = (h1_f32 * inv_rms * g_norm.astype(jnp.float32)).astype(jnp.bfloat16)
    gate_pre = jnp.dot(normed, w_gate, preferred_element_type=jnp.float32)
    up_pre = jnp.dot(normed, w_up, preferred_element_type=jnp.float32)
    mlp_act = (jax.nn.silu(gate_pre) * up_pre).astype(jnp.bfloat16)
    return (h1_f32 + jnp.dot(mlp_act, w_down, preferred_element_type=jnp.float32)).astype(jnp.bfloat16)


def seq_loss(weights, features, tokens, embedding, lm_head):
    predicted = draft_forward(weights, features, tokens, embedding)[:-1]
    target = features[1:]
    pred_error = predicted.astype(jnp.float32) - target.astype(jnp.float32)
    abs_error = jnp.abs(pred_error)
    reg_total = jnp.sum(jnp.where(abs_error < 1.0, 0.5 * pred_error * pred_error, abs_error - 0.5)) / features.shape[1]
    target_prob = jax.nn.softmax(jnp.dot(target, lm_head.T, preferred_element_type=jnp.float32), axis=-1)
    log_q = jax.nn.log_softmax(jnp.dot(predicted, lm_head.T, preferred_element_type=jnp.float32), axis=-1)
    return reg_total - CLS_WEIGHT * jnp.sum(target_prob * log_q)


def reference(features, tokens, embedding, lm_head, w_fc, b_fc, w_q, w_k, w_v, w_o, g_norm, w_gate, w_up, w_down):
    weights = (w_fc, b_fc, w_q, w_k, w_v, w_o, g_norm, w_gate, w_up, w_down)
    batch_size, seq_len = tokens.shape
    loss_and_grad = jax.value_and_grad(seq_loss)

    def scan_step(scan_carry, seq_inputs):
        loss_acc, grad_acc = scan_carry
        seq_value, seq_grads = loss_and_grad(weights, seq_inputs[0], seq_inputs[1], embedding, lm_head)
        new_grads = tuple([acc_item + grad_item.astype(jnp.float32) for acc_item, grad_item in zip(grad_acc, seq_grads)])
        return (loss_acc + seq_value, new_grads), None

    start_grads = tuple([jnp.zeros(weight_item.shape, jnp.float32) for weight_item in weights])
    final_carry, unused_out = lax.scan(scan_step, (jnp.zeros((), jnp.float32), start_grads), (features, tokens))
    loss_sum, grad_sums = final_carry
    inv_count = 1.0 / (batch_size * (seq_len - 1))
    return (loss_sum * inv_count, grad_sums[0] * inv_count, grad_sums[1] * inv_count, grad_sums[2] * inv_count, grad_sums[3] * inv_count, grad_sums[4] * inv_count, grad_sums[5] * inv_count, grad_sums[6] * inv_count, grad_sums[7] * inv_count, grad_sums[8] * inv_count, grad_sums[9] * inv_count)
```

```python
import math
import functools
import jax
import jax.numpy as jnp
from jax import lax
from jax.experimental import pallas as pl
from jax.experimental.pallas import tpu as pltpu
from jax.sharding import PartitionSpec as P

AXIS_NAME = "fsdp"
ROPE_BASE = 10000
NORM_EPS = 1e-5
CLS_WEIGHT = 0.1
F32 = jnp.float32
BF16 = jnp.bfloat16

SUB = 768
PER = 3
TILE = SUB * PER
COLS = 256
VMEM = 60 * 1024 * 1024
NEG = -1e30


def dot(a, b, ca, cb):
    return lax.dot_general(a, b, (((ca,), (cb,)), ((), ())), preferred_element_type=F32)


def rope_tables(seq_len, head_dim):
    half_dim = head_dim // 2
    inv_freq = jnp.exp(jnp.arange(half_dim, dtype=F32) * (-2.0 * math.log(ROPE_BASE) / head_dim))
    angles = jnp.arange(seq_len, dtype=F32)[:, None] * inv_freq[None, :]
    return jnp.cos(angles), jnp.sin(angles)


def apply_rope(projected, cos_tab, sin_tab):
    half_dim = projected.shape[-1] // 2
    first_half = projected[..., :half_dim]
    second_half = projected[..., half_dim:]
    cos_rows = cos_tab[None, :, None, :]
    sin_rows = sin_tab[None, :, None, :]
    return jnp.concatenate([first_half * cos_rows - second_half * sin_rows, second_half * cos_rows + first_half * sin_rows], axis=-1)


def attention_core(q_proj, k_proj, v_heads, cos_tab, sin_tab):
    batch_size, seq_len, head_count, head_dim = q_proj.shape
    kv_count = k_proj.shape[2]
    queries = apply_rope(q_proj, cos_tab, sin_tab).astype(BF16).reshape(batch_size, seq_len, kv_count, head_count // kv_count, head_dim)
    keys_rot = apply_rope(k_proj, cos_tab, sin_tab).astype(BF16)
    scores = jnp.einsum("bqkgd,bskd->bkgqs", queries, keys_rot, preferred_element_type=F32) * (1.0 / math.sqrt(head_dim))
    causal = lax.broadcasted_iota(jnp.int32, (seq_len, seq_len), 0) >= lax.broadcasted_iota(jnp.int32, (seq_len, seq_len), 1)
    attn_probs = jax.nn.softmax(jnp.where(causal, scores, -1e30), axis=-1).astype(BF16)
    attn_mixed = jnp.einsum("bkgqs,bskd->bqkgd", attn_probs, v_heads, preferred_element_type=F32).astype(BF16)
    return attn_mixed.reshape(batch_size, seq_len, head_count * head_dim)


def logits_kernel(info_ref, x_ref, h_ref, z_ref, m_ref, l_ref):
    step = pl.program_id(0)

    @pl.when(step == 0)
    def _():
        m_ref[...] = jnp.full(m_ref.shape, NEG, F32)
        l_ref[...] = jnp.zeros(l_ref.shape, F32)

    skip = jnp.where(step == 0, info_ref[1], 0)
    lane = lax.broadcasted_iota(jnp.int32, (1, 128), 1)

    def stats(c):
        parts = [z_ref[:, c * COLS + k * 128:c * COLS + (k + 1) * 128] for k in range(COLS // 128)]
        m_old = m_ref[...]
        m_new = m_old
        for part in parts:
            m_new = jnp.maximum(m_new, part)
        total = l_ref[...] * jnp.exp(m_old - m_new)
        for part in parts:
            total = total + jnp.exp(part - m_new)
        m_ref[...] = m_new
        l_ref[...] = total

    count = TILE // COLS
    for c in range(count):
        z = dot(x_ref[...], h_ref[c * COLS:(c + 1) * COLS, :], 1, 1)
        if c == 0:
            z_ref[:, :128] = jnp.where(lane < skip, NEG, z[:, :128])
            z_ref[:, 128:COLS] = z[:, 128:]
        else:
            z_ref[:, c * COLS:(c + 1) * COLS] = z
        if c > 0:
            stats(c - 1)
    stats(count - 1)


def logits_pass(info, x, lm_head, steps):
    rows, width = x.shape
    return pl.pallas_call(
        logits_kernel,
        grid_spec=pltpu.PrefetchScalarGridSpec(
            num_scalar_prefetch=1,
            grid=(steps,),
            in_specs=[pl.BlockSpec((rows, width), lambda i, s: (0, 0)),
                      pl.BlockSpec((pl.Element(TILE), pl.Element(width)), lambda i, s: (pl.multiple_of(s[0] + i * TILE, 16), 0))],
            out_specs=[pl.BlockSpec((rows, TILE), lambda i, s: (0, i)),
                       pl.BlockSpec((rows, 128), lambda i, s: (0, 0)),
                       pl.BlockSpec((rows, 128), lambda i, s: (0, 0))]),
        out_shape=[jax.ShapeDtypeStruct((rows, steps * TILE), F32),
                   jax.ShapeDtypeStruct((rows, 128), F32),
                   jax.ShapeDtypeStruct((rows, 128), F32)],
        compiler_params=pltpu.CompilerParams(dimension_semantics=("arbitrary",), vmem_limit_bytes=VMEM),
        cost_estimate=pl.CostEstimate(flops=2 * rows * width * steps * TILE, bytes_accessed=steps * TILE * (2 * width + 4 * rows),
                                      transcendentals=2 * rows * steps * TILE),
        name="vocab_logits",
    )(info, x, lm_head)


def grad_kernel(steps, info_ref, zt_ref, zq_ref, ha_ref, hb_ref, hc_ref, lt_ref, lq_ref, scale_ref, dy_ref, cross_ref, ga, gb, gc):
    step = pl.program_id(0)

    def fill(g_ref, index):
        part_cross = jnp.zeros(cross_ref.shape, F32)
        for k in range(SUB // 128):
            cols = slice(index * SUB + k * 128, index * SUB + (k + 1) * 128)
            log_q = zq_ref[:, cols] - lq_ref[...]
            prob = jnp.exp(zt_ref[:, cols] - lt_ref[...])
            part_cross = part_cross + prob * log_q
            g_ref[:, k * 128:(k + 1) * 128] = ((jnp.exp(log_q) - prob) * scale_ref[...]).astype(BF16)
        cross_ref[...] += part_cross

    @pl.when(step == 0)
    def _():
        dy_ref[...] = jnp.zeros(dy_ref.shape, F32)
        cross_ref[...] = jnp.zeros(cross_ref.shape, F32)
        gc[...] = jnp.zeros(gc.shape, BF16)

    @pl.when(step < steps)
    def _():
        dy_ref[...] += dot(gc[...], ha_ref[...], 1, 0)
        fill(ga, 0)
        dy_ref[...] += dot(ga[...], hb_ref[...], 1, 0)
        fill(gb, 1)
        dy_ref[...] += dot(gb[...], hc_ref[...], 1, 0)
        fill(gc, 2)

    @pl.when(step == steps)
    def _():
        dy_ref[...] += dot(gc[...], ha_ref[...], 1, 0)


def grad_pass(info, zt, zq, lm_head, lse_t, lse_q, scale, steps):
    rows = zt.shape[0]
    width = lm_head.shape[1]
    last = steps * PER - 1

    def head_spec(shift):
        return pl.BlockSpec((pl.Element(SUB), pl.Element(width)),
                            lambda i, s: (pl.multiple_of(s[0] + jnp.clip(i * PER + shift, 0, last) * SUB, 16), 0))

    z_spec = pl.BlockSpec((rows, TILE), lambda i, s: (0, jnp.minimum(i, steps - 1)))
    row_spec = pl.BlockSpec((rows, 128), lambda i, s: (0, 0))
    return pl.pallas_call(
        functools.partial(grad_kernel, steps),
        grid_spec=pltpu.PrefetchScalarGridSpec(
            num_scalar_prefetch=1,
            grid=(steps + 1,),
            in_specs=[z_spec, z_spec, head_spec(-1), head_spec(0), head_spec(1), row_spec, row_spec, row_spec],
            out_specs=[pl.BlockSpec((rows, width), lambda i, s: (0, 0)), row_spec],
            scratch_shapes=[pltpu.VMEM((rows, SUB), BF16)] * PER),
        out_shape=[jax.ShapeDtypeStruct((rows, width), F32), jax.ShapeDtypeStruct((rows, 128), F32)],
        compiler_params=pltpu.CompilerParams(dimension_semantics=("arbitrary",), vmem_limit_bytes=VMEM),
        cost_estimate=pl.CostEstimate(flops=2 * rows * width * steps * TILE, bytes_accessed=steps * TILE * (2 * width + 8 * rows),
                                      transcendentals=2 * rows * steps * TILE),
        name="vocab_grad",
    )(info, zt, zq, lm_head, lm_head, lm_head, lse_t, lse_q, scale)


def lane_lse(m, l):
    top = jnp.max(m, axis=1, keepdims=True)
    return top, jnp.sum(l * jnp.exp(m - top), axis=1, keepdims=True)


def solution(mesh):
    n = mesh.shape[AXIS_NAME]
    split_spec = P(AXIS_NAME)
    whole_spec = P()
    pair = [(i, i ^ 1) for i in range(n)]

    def gather(x):
        return lax.all_gather(x, AXIS_NAME, axis=0, tiled=True)

    def swap(x):
        return lax.ppermute(x, AXIS_NAME, pair)

    def spread(x):
        return lax.all_to_all(x, AXIS_NAME, 0, 0, tiled=True)

    def by_owner(x):
        return x.reshape(x.shape[0], n, x.shape[1] // n).transpose(1, 0, 2)

    def local_step(features, tokens, embedding, lm_head, w_fc, b_fc, w_q, w_k, w_v, w_o, g_norm, w_gate, w_up, w_down):
        batch, seq, width = features.shape
        rows = batch * seq
        vocab = lm_head.shape[0]
        heads, head_dim = w_q.shape[1:]
        kvs = w_k.shape[1]
        qw, kw = heads * head_dim, kvs * head_dim
        shard = w_q.shape[0]
        hidden = w_gate.shape[1]
        inv_count = 1.0 / (batch * n * (seq - 1))
        me = lax.axis_index(AXIS_NAME)
        core = lax.rem(me, 2)

        per_group = hidden // 128 // (n // 4)
        wide = -(-per_group // 4) * 128
        starts = [128 * per_group * (j // 4) + wide * (j % 4) for j in range(n)]
        ends = [starts[j + 1] if j + 1 < n else hidden for j in range(n)]
        spare = starts[-1] + wide - hidden
        place = lax.rem(me, 4)
        shift = wide - hidden // n

        steps = -(-(vocab // 2) // TILE)
        span = steps * TILE
        info = jnp.stack([jnp.where(core == 0, 0, vocab - span), jnp.where(core == 0, 0, 2 * span - vocab)]).astype(jnp.int32)

        f_rows = features.reshape(rows, width)

        def next_rows(x):
            x = x.reshape(batch, seq, width)
            return jnp.concatenate([x[:, 1:], x[:, -1:]], axis=1).reshape(rows, width)

        target = jnp.concatenate([next_rows(f_rows), next_rows(swap(f_rows))], axis=0)
        fc_full = gather(w_fc)
        small = jnp.pad(jnp.stack([b_fc, g_norm], axis=1), ((0, 0), (0, 126)))
        packed = gather(jnp.concatenate([w_q.reshape(shard, qw), w_k.reshape(shard, kw), w_v.reshape(shard, kw), small, w_o], axis=1))
        qkv_full = packed[:, :qw + 2 * kw]
        bias = packed[:, qw + 2 * kw].astype(F32)
        gain = packed[:, qw + 2 * kw + 1].astype(F32)
        o_full = packed[:, qw + 2 * kw + 128:]

        def tiles(w):
            w = jnp.pad(w, ((0, 0), (0, spare)))
            return jnp.stack([w[:, s:s + wide] for s in starts])

        gu = spread(jnp.concatenate([tiles(w_gate), tiles(w_up)], axis=2)).reshape(width, 2 * wide)
        up_rows = lax.ppermute(w_down[:128], AXIS_NAME, [(j + 1, j) for j in range(n - 1) if j % 4 != 3])
        down = lax.dynamic_slice(jnp.concatenate([w_down, up_rows], axis=0), (shift * place, 0), (wide, width))

        zt, m_t, l_t = logits_pass(info, target, lm_head, steps)
        fc_full, zt, m_t, l_t = lax.optimization_barrier((fc_full, zt, m_t, l_t))

        emb_rows = embedding[tokens].reshape(rows, width)
        hidden0 = (dot(f_rows, fc_full[:width], 1, 0) + dot(emb_rows, fc_full[width:], 1, 0) + bias).astype(BF16)
        qkv = dot(hidden0, qkv_full, 1, 0)
        q_proj = qkv[:, :qw].reshape(batch, seq, heads, head_dim)
        k_proj = qkv[:, qw:qw + kw].reshape(batch, seq, kvs, head_dim)
        v_heads = qkv[:, qw + kw:].astype(BF16).reshape(batch, seq, kvs, head_dim)
        cos_tab, sin_tab = rope_tables(seq, head_dim)
        attn_fn = functools.partial(attention_core, cos_tab=cos_tab, sin_tab=sin_tab)
        mixed, attn_vjp = jax.vjp(attn_fn, q_proj, k_proj, v_heads)
        mixed_rows = mixed.reshape(rows, qw)
        hidden1 = (hidden0.astype(F32) + dot(mixed_rows, o_full, 1, 0)).astype(BF16)
        h1 = hidden1.astype(F32)
        inv_rms = lax.rsqrt(jnp.mean(h1 * h1, axis=-1, keepdims=True) + NORM_EPS)
        normed = (h1 * inv_rms * gain).astype(BF16)

        normed_all = gather(normed)
        pre = dot(normed_all, gu, 1, 0)
        gate_pre, up_pre = pre[:, :wide], pre[:, wide:]
        gate_sig = jax.nn.sigmoid(gate_pre)
        gate_act = gate_pre * gate_sig
        act = (gate_act * up_pre).astype(BF16)
        mlp_out = lax.psum_scatter(dot(act, down, 1, 0), AXIS_NAME, scatter_dimension=0, tiled=True)
        draft_out = (h1 + mlp_out).astype(BF16)

        draft_pair = jnp.concatenate([draft_out, swap(draft_out)], axis=0)
        zq, m_q, l_q = logits_pass(info, draft_pair, lm_head, steps)
        inputs_all = spread(jnp.concatenate([by_owner(jnp.concatenate([f_rows, emb_rows], axis=1)), by_owner(hidden0), by_owner(mixed_rows)], axis=2))
        inputs_all = inputs_all.reshape(n * rows, 4 * shard)
        top_t, sum_t = lane_lse(m_t, l_t)
        top_q, sum_q = lane_lse(m_q, l_q)
        mine = jnp.concatenate([top_t, sum_t, top_q, sum_q], axis=1)
        theirs = swap(mine)
        theirs = jnp.concatenate([theirs[rows:], theirs[:rows]], axis=0)

        def merged(k):
            top = jnp.maximum(mine[:, k], theirs[:, k])
            total = mine[:, k + 1] * jnp.exp(mine[:, k] - top) + theirs[:, k + 1] * jnp.exp(theirs[:, k] - top)
            return top + jnp.log(total)

        valid = (lax.rem(lax.broadcasted_iota(jnp.int32, (2 * rows, 1), 0), seq) < seq - 1).astype(F32)

        def lanes(x):
            return jnp.broadcast_to(x.reshape(2 * rows, 1), (2 * rows, 128))

        dy, cross = grad_pass(info, zt, zq, lm_head, lanes(merged(0)), lanes(merged(2)), lanes(valid * (CLS_WEIGHT * inv_count)), steps)
        dy, inputs_all = lax.optimization_barrier((dy, inputs_all))
        dy_own = dy[:rows] + swap(dy[rows:])

        error = (draft_out.astype(F32) - next_rows(f_rows).astype(F32)) * valid[:rows]
        abs_error = jnp.abs(error)
        reg_total = jnp.sum(jnp.where(abs_error < 1.0, 0.5 * error * error, abs_error - 0.5)) / width
        local_loss = reg_total - CLS_WEIGHT * jnp.sum(cross * valid)

        d_out = (jnp.clip(error, -1.0, 1.0) * (inv_count / width) + dy_own) * valid[:rows]
        d_out_all = gather(d_out.astype(BF16))
        d_act = dot(d_out_all, down, 1, 1)
        d_gate = (d_act * up_pre * gate_sig * (1.0 + gate_pre * (1.0 - gate_sig))).astype(BF16)
        d_up = (d_act * gate_act).astype(BF16)
        d_gu = jnp.concatenate([d_gate, d_up], axis=1)
        d_normed = lax.psum_scatter(dot(d_gu, gu, 1, 1), AXIS_NAME, scatter_dimension=0, tiled=True)
        grad_gu = dot(normed_all, d_gu, 0, 0).reshape(n, shard, 2 * wide)
        d_normed, grad_gu = lax.optimization_barrier((d_normed, grad_gu))
        grad_gu = spread(grad_gu)
        grad_gate = jnp.concatenate([grad_gu[j][:, :ends[j] - starts[j]] for j in range(n)], axis=1)
        grad_up = jnp.concatenate([grad_gu[j][:, wide:wide + ends[j] - starts[j]] for j in range(n)], axis=1)
        grad_down = dot(act, d_out_all, 0, 0)
        edge = 3 * shift
        from_prev = lax.ppermute(grad_down[wide - edge:], AXIS_NAME, [(j, j + 1) for j in range(n - 1) if j % 4 != 3])
        grad_down = lax.dynamic_slice(jnp.concatenate([from_prev, grad_down], axis=0), (edge - shift * place, 0), (hidden // n, width))

        gained = d_normed * gain
        d_hidden1 = d_out + inv_rms * gained - h1 * (inv_rms * inv_rms * inv_rms) * jnp.mean(gained * h1, axis=-1, keepdims=True)
        d_h1 = d_hidden1.astype(BF16)
        sums = lax.psum(jnp.concatenate([jnp.sum(d_normed * h1 * inv_rms, axis=0), jnp.full((128,), local_loss, F32)]), AXIS_NAME)
        total_loss = sums[width] * inv_count
        grad_gain = lax.dynamic_slice(sums, (me * shard,), (shard,))
        d_h1_all = gather(d_h1)
        d_mixed = dot(d_h1, o_full, 1, 1).astype(BF16)
        d_q, d_k, d_v = attn_vjp(d_mixed.reshape(mixed.shape))
        d_qkv = jnp.concatenate([d_q.reshape(rows, qw).astype(BF16), d_k.reshape(rows, kw).astype(BF16), d_v.reshape(rows, kw)], axis=1)
        d_h0 = (d_hidden1 + dot(d_qkv, qkv_full, 1, 1)).astype(BF16)
        d_qkv_all = gather(d_qkv)
        d_h0_all = gather(d_h0)
        grad_o = dot(inputs_all[:, 3 * shard:], d_h1_all, 0, 0)
        grad_qkv = dot(inputs_all[:, 2 * shard:3 * shard], d_qkv_all, 0, 0)
        grad_fc = dot(inputs_all[:, :2 * shard], d_h0_all, 0, 0)
        grad_bias = jnp.sum(lax.dynamic_slice(d_h0_all, (0, me * shard), (n * rows, shard)).astype(F32), axis=0)
        return (total_loss, grad_fc, grad_bias, grad_qkv[:, :qw].reshape(w_q.shape), grad_qkv[:, qw:qw + kw].reshape(w_k.shape),
                grad_qkv[:, qw + kw:].reshape(w_v.shape), grad_o, grad_gain, grad_gate, grad_up, grad_down)

    return jax.shard_map(local_step, mesh=mesh, in_specs=(split_spec, split_spec, whole_spec, whole_spec) + (split_spec,) * 10,
                         out_specs=(whole_spec,) + (split_spec,) * 10, check_vma=False)
```

```python
import math
import functools
import jax
import jax.numpy as jnp
from jax import lax
from jax.experimental import pallas as pl
from jax.experimental.pallas import tpu as pltpu
from jax.sharding import PartitionSpec as P

AXIS_NAME = "fsdp"
ROPE_BASE = 10000
NORM_EPS = 1e-5
CLS_WEIGHT = 0.1
F32 = jnp.float32
BF16 = jnp.bfloat16

SUB = 768
PER = 3
TILE = SUB * PER
COLS = 256
VMEM = 60 * 1024 * 1024
NEG = -1e30


def dot(a, b, ca, cb):
    return lax.dot_general(a, b, (((ca,), (cb,)), ((), ())), preferred_element_type=F32)


def rope_tables(seq_len, head_dim):
    half_dim = head_dim // 2
    inv_freq = jnp.exp(jnp.arange(half_dim, dtype=F32) * (-2.0 * math.log(ROPE_BASE) / head_dim))
    angles = jnp.arange(seq_len, dtype=F32)[:, None] * inv_freq[None, :]
    return jnp.cos(angles), jnp.sin(angles)


def apply_rope(projected, cos_tab, sin_tab):
    half_dim = projected.shape[-1] // 2
    first_half = projected[..., :half_dim]
    second_half = projected[..., half_dim:]
    cos_rows = cos_tab[None, :, None, :]
    sin_rows = sin_tab[None, :, None, :]
    return jnp.concatenate([first_half * cos_rows - second_half * sin_rows, second_half * cos_rows + first_half * sin_rows], axis=-1)


def attention_core(q_proj, k_proj, v_heads, cos_tab, sin_tab):
    batch_size, seq_len, head_count, head_dim = q_proj.shape
    kv_count = k_proj.shape[2]
    queries = apply_rope(q_proj, cos_tab, sin_tab).astype(BF16).reshape(batch_size, seq_len, kv_count, head_count // kv_count, head_dim)
    keys_rot = apply_rope(k_proj, cos_tab, sin_tab).astype(BF16)
    scores = jnp.einsum("bqkgd,bskd->bkgqs", queries, keys_rot, preferred_element_type=F32) * (1.0 / math.sqrt(head_dim))
    causal = lax.broadcasted_iota(jnp.int32, (seq_len, seq_len), 0) >= lax.broadcasted_iota(jnp.int32, (seq_len, seq_len), 1)
    attn_probs = jax.nn.softmax(jnp.where(causal, scores, -1e30), axis=-1).astype(BF16)
    attn_mixed = jnp.einsum("bkgqs,bskd->bqkgd", attn_probs, v_heads, preferred_element_type=F32).astype(BF16)
    return attn_mixed.reshape(batch_size, seq_len, head_count * head_dim)


def logits_kernel(info_ref, x_ref, ha_ref, hb_ref, hc_ref, z_ref, m_ref, l_ref):
    step = pl.program_id(0)

    @pl.when(step == 0)
    def _():
        m_ref[...] = jnp.full(m_ref.shape, NEG, F32)
        l_ref[...] = jnp.zeros(l_ref.shape, F32)

    skip = jnp.where(step == 0, info_ref[1], 0)
    lane = lax.broadcasted_iota(jnp.int32, (1, 128), 1)

    def stats(c):
        parts = [z_ref[:, c * COLS + k * 128:c * COLS + (k + 1) * 128] for k in range(COLS // 128)]
        m_old = m_ref[...]
        m_new = m_old
        for part in parts:
            m_new = jnp.maximum(m_new, part)
        total = l_ref[...] * jnp.exp(m_old - m_new)
        for part in parts:
            total = total + jnp.exp(part - m_new)
        m_ref[...] = m_new
        l_ref[...] = total

    count = TILE // COLS
    for c in range(count):
        h_ref, part = (ha_ref, hb_ref, hc_ref)[c * COLS // SUB], c % (SUB // COLS)
        z = dot(x_ref[...], h_ref[part * COLS:(part + 1) * COLS, :], 1, 1)
        if c == 0:
            z_ref[:, :128] = jnp.where(lane < skip, NEG, z[:, :128])
            z_ref[:, 128:COLS] = z[:, 128:]
        else:
            z_ref[:, c * COLS:(c + 1) * COLS] = z
        if c > 0:
            stats(c - 1)
    stats(count - 1)


def logits_pass(info, x, lm_head, steps):
    rows, width = x.shape
    return pl.pallas_call(
        logits_kernel,
        grid_spec=pltpu.PrefetchScalarGridSpec(
            num_scalar_prefetch=1,
            grid=(steps,),
            in_specs=[pl.BlockSpec((rows, width), lambda i, s: (0, 0))] + [
                pl.BlockSpec((pl.Element(SUB), pl.Element(width)), lambda i, s, k=k: (pl.multiple_of(s[0] + i * TILE + k * SUB, 16), 0))
                for k in range(PER)],
            out_specs=[pl.BlockSpec((rows, TILE), lambda i, s: (0, i)),
                       pl.BlockSpec((rows, 128), lambda i, s: (0, 0)),
                       pl.BlockSpec((rows, 128), lambda i, s: (0, 0))]),
        out_shape=[jax.ShapeDtypeStruct((rows, steps * TILE), F32),
                   jax.ShapeDtypeStruct((rows, 128), F32),
                   jax.ShapeDtypeStruct((rows, 128), F32)],
        compiler_params=pltpu.CompilerParams(dimension_semantics=("arbitrary",), vmem_limit_bytes=VMEM),
        cost_estimate=pl.CostEstimate(flops=2 * rows * width * steps * TILE, bytes_accessed=steps * TILE * (2 * width + 4 * rows),
                                      transcendentals=2 * rows * steps * TILE),
        name="vocab_logits",
    )(info, x, lm_head, lm_head, lm_head)


def grad_kernel(steps, info_ref, zt_ref, zq_ref, ha_ref, hb_ref, hc_ref, lt_ref, lq_ref, scale_ref, dy_ref, cross_ref, ga, gb, gc):
    step = pl.program_id(0)

    def fill(g_ref, index):
        part_cross = jnp.zeros(cross_ref.shape, F32)
        for k in range(SUB // 128):
            cols = slice(index * SUB + k * 128, index * SUB + (k + 1) * 128)
            log_q = zq_ref[:, cols] - lq_ref[...]
            prob = jnp.exp(zt_ref[:, cols] - lt_ref[...])
            part_cross = part_cross + prob * log_q
            g_ref[:, k * 128:(k + 1) * 128] = ((jnp.exp(log_q) - prob) * scale_ref[...]).astype(BF16)
        cross_ref[...] += part_cross

    @pl.when(step == 0)
    def _():
        dy_ref[...] = jnp.zeros(dy_ref.shape, F32)
        cross_ref[...] = jnp.zeros(cross_ref.shape, F32)
        gc[...] = jnp.zeros(gc.shape, BF16)

    @pl.when(step < steps)
    def _():
        dy_ref[...] += dot(gc[...], ha_ref[...], 1, 0)
        fill(ga, 0)
        dy_ref[...] += dot(ga[...], hb_ref[...], 1, 0)
        fill(gb, 1)
        dy_ref[...] += dot(gb[...], hc_ref[...], 1, 0)
        fill(gc, 2)

    @pl.when(step == steps)
    def _():
        dy_ref[...] += dot(gc[...], ha_ref[...], 1, 0)


def grad_pass(info, zt, zq, lm_head, lse_t, lse_q, scale, steps):
    rows = zt.shape[0]
    width = lm_head.shape[1]
    last = steps * PER - 1

    def head_spec(shift):
        return pl.BlockSpec((pl.Element(SUB), pl.Element(width)),
                            lambda i, s: (pl.multiple_of(s[0] + jnp.clip(i * PER + shift, 0, last) * SUB, 16), 0))

    z_spec = pl.BlockSpec((rows, TILE), lambda i, s: (0, jnp.minimum(i, steps - 1)))
    row_spec = pl.BlockSpec((rows, 128), lambda i, s: (0, 0))
    return pl.pallas_call(
        functools.partial(grad_kernel, steps),
        grid_spec=pltpu.PrefetchScalarGridSpec(
            num_scalar_prefetch=1,
            grid=(steps + 1,),
            in_specs=[z_spec, z_spec, head_spec(-1), head_spec(0), head_spec(1), row_spec, row_spec, row_spec],
            out_specs=[pl.BlockSpec((rows, width), lambda i, s: (0, 0)), row_spec],
            scratch_shapes=[pltpu.VMEM((rows, SUB), BF16)] * PER),
        out_shape=[jax.ShapeDtypeStruct((rows, width), F32), jax.ShapeDtypeStruct((rows, 128), F32)],
        compiler_params=pltpu.CompilerParams(dimension_semantics=("arbitrary",), vmem_limit_bytes=VMEM),
        cost_estimate=pl.CostEstimate(flops=2 * rows * width * steps * TILE, bytes_accessed=steps * TILE * (2 * width + 8 * rows),
                                      transcendentals=2 * rows * steps * TILE),
        name="vocab_grad",
    )(info, zt, zq, lm_head, lm_head, lm_head, lse_t, lse_q, scale)


def exchange_kernel(compute, n_inputs, n_outputs, reduced, *refs):
    own, inputs = refs[0], refs[1:n_inputs]
    blocks, out = refs[n_inputs], refs[n_inputs + 1]
    outputs = refs[n_inputs + 2:n_inputs + n_outputs]
    part, pair_in, relay_x, relay_y, from_x, from_y, gsend, grecv, dsend, drecv, ssend, srecv = refs[n_inputs + n_outputs:n_inputs + n_outputs + 12]
    rows = own.shape[0]
    half = rows // 2
    me = lax.axis_index(AXIS_NAME)
    core, x, y = me % 2, (me // 2) % 2, me // 4
    mate = me + 1 - 2 * core
    xn = me + 2 - 4 * x
    yn = me + 4 - 8 * y

    def remote(src, dst, send, recv, to):
        return pltpu.make_async_remote_copy(src_ref=src, dst_ref=dst, send_sem=send, recv_sem=recv, device_id=(to,),
                                            device_id_type=pl.DeviceIdType.MESH)

    def slot(s, first=0, count=rows):
        return blocks.at[pl.ds(s * rows + first, count)]

    to_mate = remote(own, slot(1), gsend.at[0], grecv.at[0], mate)
    to_x = remote(own, slot(2), gsend.at[1], grecv.at[1], xn)
    to_y = remote(own, slot(4), gsend.at[2], grecv.at[2], yn)
    x_to_y = remote(slot(2, 0, half), slot(6, 0, half), gsend.at[3], grecv.at[3], yn)
    y_to_x = remote(slot(4, half, half), slot(6, half, half), gsend.at[4], grecv.at[4], xn)
    x_to_mate = remote(slot(2), slot(3), gsend.at[5], grecv.at[5], mate)
    y_to_mate = remote(slot(4), slot(5), gsend.at[6], grecv.at[6], mate)
    d_to_mate = remote(slot(6), slot(7), gsend.at[7], grecv.at[7], mate)
    pair = [remote(part.at[2 * k + 1], pair_in.at[k], dsend.at[k], drecv.at[k], mate) for k in range(4)]
    top, bottom = pl.ds(0, half), pl.ds(half, half)
    diag_x = remote(part.at[6, top], relay_x, ssend.at[0], srecv.at[0], xn)
    diag_y = remote(part.at[6, bottom], relay_y, ssend.at[1], srecv.at[1], yn)
    x_top = remote(part.at[2, top], from_x.at[top], ssend.at[2], srecv.at[2], xn)
    x_bottom = remote(part.at[2, bottom], from_x.at[bottom], ssend.at[3], srecv.at[3], xn)
    y_top = remote(part.at[4, top], from_y.at[top], ssend.at[4], srecv.at[4], yn)
    y_bottom = remote(part.at[4, bottom], from_y.at[bottom], ssend.at[5], srecv.at[5], yn)

    barrier = pltpu.get_barrier_semaphore()
    for other in (mate, xn, yn):
        pl.semaphore_signal(barrier, inc=1, device_id=(other,), device_id_type=pl.DeviceIdType.MESH)
    blocks[pl.ds(0, rows)] = own[...]
    pl.semaphore_wait(barrier, 3)
    to_x.start()
    to_y.start()
    to_mate.start()

    def body(s, carry):
        @pl.when(s == 1)
        def _():
            to_mate.wait_recv()

        @pl.when(s == 2)
        def _():
            to_x.wait_recv()
            x_to_y.start()
            x_to_mate.start()
            to_y.wait_recv()
            y_to_x.start()
            y_to_mate.start()

        @pl.when(s == 3)
        def _():
            x_to_mate.wait_recv()

        @pl.when(s == 5)
        def _():
            y_to_mate.wait_recv()

        @pl.when(s == 6)
        def _():
            x_to_y.wait_recv()
            y_to_x.wait_recv()
            d_to_mate.start()

        @pl.when(s == 7)
        def _():
            d_to_mate.wait_recv()

        compute(s, blocks, part, inputs, outputs)

        @pl.when(s == 1)
        def _():
            pair[0].start()

        @pl.when(s == 3)
        def _():
            pair[1].start()

        @pl.when(s == 4)
        def _():
            pair[1].wait_recv()
            part[2] += pair_in[1]
            x_top.start()

        @pl.when(s == 5)
        def _():
            pair[2].start()

        @pl.when(s == 6)
        def _():
            pair[2].wait_recv()
            part[4] += pair_in[2]
            y_bottom.start()

        return carry

    lax.fori_loop(0, 8, body, 0)
    pair[3].start()
    pair[3].wait_recv()
    part[6] += pair_in[3]
    diag_x.start()
    diag_y.start()
    pair[0].wait_recv()
    part[0] += pair_in[0]
    diag_y.wait_recv()
    part[2, bottom] += relay_y[...]
    x_bottom.start()
    diag_x.wait_recv()
    part[4, top] += relay_x[...]
    y_top.start()
    x_top.wait_recv()
    y_bottom.wait_recv()
    x_bottom.wait_recv()
    y_top.wait_recv()
    out[...] = part[0] + from_x[...] + from_y[...]
    small = []
    if reduced:
        scaled, scalar = inputs[-2:]
        sums = outputs[-1]
        mine, theirs, rsend, rrecv = refs[n_inputs + n_outputs + 12:]
        mine[0, :, :scaled.shape[1]] = jnp.broadcast_to(jnp.sum(out[...] * scaled[...], axis=0, keepdims=True), (8, scaled.shape[1]))
        mine[0, :, scaled.shape[1]:] = scalar[...]
        for k, other in enumerate((mate, xn, yn)):
            copy = remote(mine.at[k], theirs.at[k], rsend.at[k], rrecv.at[k], other)
            copy.start()
            copy.wait_recv()
            small.append(copy)
            if k < 2:
                mine[k + 1] = mine[k] + theirs[k]
            else:
                sums[...] = mine[k] + theirs[k]
    for copy in small + [to_mate, to_x, to_y, x_to_y, y_to_x, x_to_mate, y_to_mate, d_to_mate] + pair + [diag_x, diag_y, x_top, x_bottom, y_top, y_bottom]:
        copy.wait_send()


CHUNK = 384


def forward_block(s, blocks, part, inputs, outputs):
    gu, down = inputs
    act, = outputs
    wide = down.shape[0]
    rows = part.shape[1]
    here = pl.ds(pl.multiple_of(s * rows, rows), rows)
    for c in range(0, wide, CHUNK):
        gate = dot(blocks[here], gu[:, c:c + CHUNK], 1, 0)
        up = dot(blocks[here], gu[:, wide + c:wide + c + CHUNK], 1, 0)
        act[here, c:c + CHUNK] = (gate * jax.nn.sigmoid(gate) * up).astype(BF16)
    part[s] = dot(act[here], down[...], 1, 0)


def backward_block(s, blocks, part, inputs, outputs):
    gu, down, normed = inputs[:3]
    d_gu = outputs[0]
    wide = down.shape[0]
    rows = part.shape[1]
    here = pl.ds(pl.multiple_of(s * rows, rows), rows)
    for c in range(0, wide, CHUNK):
        gate = dot(normed[here], gu[:, c:c + CHUNK], 1, 0)
        up = dot(normed[here], gu[:, wide + c:wide + c + CHUNK], 1, 0)
        d_act = dot(blocks[here], down[c:c + CHUNK], 1, 1)
        sig = jax.nn.sigmoid(gate)
        d_gu[here, c:c + CHUNK] = (d_act * up * sig * (1.0 + gate * (1.0 - sig))).astype(BF16)
        d_gu[here, wide + c:wide + c + CHUNK] = (d_act * (gate * sig)).astype(BF16)
    part[s] = dot(d_gu[here], gu[...], 1, 1)


def exchange(compute, collective_id, own, inputs, extra_shape, products, reduced=False):
    rows, width = own.shape
    vmem = pl.BlockSpec(memory_space=pltpu.VMEM)
    n_inputs = 1 + len(inputs)
    n_outputs = 4 if reduced else 3
    shapes = [jax.ShapeDtypeStruct((8 * rows, width), BF16), jax.ShapeDtypeStruct((rows, width), F32), jax.ShapeDtypeStruct(extra_shape, BF16)]
    scratch = []
    if reduced:
        shapes.append(jax.ShapeDtypeStruct((8, width + 128), F32))
        scratch = [pltpu.VMEM((3, 8, width + 128), F32), pltpu.VMEM((3, 8, width + 128), F32), pltpu.SemaphoreType.DMA((3,)),
                   pltpu.SemaphoreType.DMA((3,))]
    return pl.pallas_call(
        functools.partial(exchange_kernel, compute, n_inputs, n_outputs, reduced),
        in_specs=[vmem] * n_inputs,
        out_specs=[vmem] * n_outputs,
        out_shape=shapes,
        scratch_shapes=[pltpu.VMEM((8, rows, width), F32), pltpu.VMEM((4, rows, width), F32),
                        pltpu.VMEM((rows // 2, width), F32), pltpu.VMEM((rows // 2, width), F32),
                        pltpu.VMEM((rows, width), F32), pltpu.VMEM((rows, width), F32),
                        pltpu.SemaphoreType.DMA((8,)), pltpu.SemaphoreType.DMA((8,)), pltpu.SemaphoreType.DMA((4,)),
                        pltpu.SemaphoreType.DMA((4,)), pltpu.SemaphoreType.DMA((6,)), pltpu.SemaphoreType.DMA((6,))] + scratch,
        compiler_params=pltpu.CompilerParams(collective_id=collective_id, has_side_effects=True, vmem_limit_bytes=VMEM),
        cost_estimate=pl.CostEstimate(flops=products * 2 * 8 * rows * width * extra_shape[1] // 2, bytes_accessed=40_000_000, transcendentals=0),
    )(own, *inputs)


def lane_lse(m, l):
    top = jnp.max(m, axis=1, keepdims=True)
    return top, jnp.sum(l * jnp.exp(m - top), axis=1, keepdims=True)


def solution(mesh):
    n = mesh.shape[AXIS_NAME]
    split_spec = P(AXIS_NAME)
    whole_spec = P()
    pair = [(i, i ^ 1) for i in range(n)]

    def gather(x):
        return lax.all_gather(x, AXIS_NAME, axis=0, tiled=True)

    def swap(x):
        return lax.ppermute(x, AXIS_NAME, pair)

    def spread(x):
        return lax.all_to_all(x, AXIS_NAME, 0, 0, tiled=True)

    def by_owner(x):
        return x.reshape(x.shape[0], n, x.shape[1] // n).transpose(1, 0, 2)

    def local_step(features, tokens, embedding, lm_head, w_fc, b_fc, w_q, w_k, w_v, w_o, g_norm, w_gate, w_up, w_down):
        batch, seq, width = features.shape
        rows = batch * seq
        vocab = lm_head.shape[0]
        heads, head_dim = w_q.shape[1:]
        kvs = w_k.shape[1]
        qw, kw = heads * head_dim, kvs * head_dim
        shard = w_q.shape[0]
        hidden = w_gate.shape[1]
        inv_count = 1.0 / (batch * n * (seq - 1))
        me = lax.axis_index(AXIS_NAME)
        core = lax.rem(me, 2)

        per_group = hidden // 128 // (n // 4)
        wide = -(-per_group // 4) * 128
        starts = [128 * per_group * (j // 4) + wide * (j % 4) for j in range(n)]
        ends = [starts[j + 1] if j + 1 < n else hidden for j in range(n)]
        spare = starts[-1] + wide - hidden
        place = lax.rem(me, 4)
        shift = wide - hidden // n

        steps = -(-(vocab // 2) // TILE)
        span = steps * TILE
        info = jnp.stack([jnp.where(core == 0, 0, vocab - span), jnp.where(core == 0, 0, 2 * span - vocab)]).astype(jnp.int32)

        f_rows = features.reshape(rows, width)

        def next_rows(x):
            x = x.reshape(batch, seq, width)
            return jnp.concatenate([x[:, 1:], x[:, -1:]], axis=1).reshape(rows, width)

        target = jnp.concatenate([next_rows(f_rows), next_rows(swap(f_rows))], axis=0)
        fc_full = gather(w_fc)
        small = jnp.pad(jnp.stack([b_fc, g_norm], axis=1), ((0, 0), (0, 126)))
        packed = gather(jnp.concatenate([w_q.reshape(shard, qw), w_k.reshape(shard, kw), w_v.reshape(shard, kw), small, w_o], axis=1))
        qkv_full = packed[:, :qw + 2 * kw]
        bias = packed[:, qw + 2 * kw].astype(F32)
        gain = packed[:, qw + 2 * kw + 1].astype(F32)
        o_full = packed[:, qw + 2 * kw + 128:]

        def tiles(w):
            w = jnp.pad(w, ((0, 0), (0, spare)))
            return jnp.stack([w[:, s:s + wide] for s in starts])

        gu = spread(jnp.concatenate([tiles(w_gate), tiles(w_up)], axis=2)).reshape(width, 2 * wide)
        up_rows = lax.ppermute(w_down[:128], AXIS_NAME, [(j + 1, j) for j in range(n - 1) if j % 4 != 3])
        down = lax.dynamic_slice(jnp.concatenate([w_down, up_rows], axis=0), (shift * place, 0), (wide, width))

        zt, m_t, l_t = logits_pass(info, target, lm_head, steps)
        fc_full, zt, m_t, l_t = lax.optimization_barrier((fc_full, zt, m_t, l_t))

        emb_rows = embedding[tokens].reshape(rows, width)
        hidden0 = (dot(f_rows, fc_full[:width], 1, 0) + dot(emb_rows, fc_full[width:], 1, 0) + bias).astype(BF16)
        qkv = dot(hidden0, qkv_full, 1, 0)
        q_proj = qkv[:, :qw].reshape(batch, seq, heads, head_dim)
        k_proj = qkv[:, qw:qw + kw].reshape(batch, seq, kvs, head_dim)
        v_heads = qkv[:, qw + kw:].astype(BF16).reshape(batch, seq, kvs, head_dim)
        cos_tab, sin_tab = rope_tables(seq, head_dim)
        attn_fn = functools.partial(attention_core, cos_tab=cos_tab, sin_tab=sin_tab)
        mixed, attn_vjp = jax.vjp(attn_fn, q_proj, k_proj, v_heads)
        mixed_rows = mixed.reshape(rows, qw)
        hidden1 = (hidden0.astype(F32) + dot(mixed_rows, o_full, 1, 0)).astype(BF16)
        h1 = hidden1.astype(F32)
        inv_rms = lax.rsqrt(jnp.mean(h1 * h1, axis=-1, keepdims=True) + NORM_EPS)
        normed = (h1 * inv_rms * gain).astype(BF16)

        normed_all, mlp_out, act = exchange(forward_block, 1, normed, (gu, down), (n * rows, wide), 3)
        draft_out = (h1 + mlp_out).astype(BF16)

        draft_pair = jnp.concatenate([draft_out, swap(draft_out)], axis=0)
        zq, m_q, l_q = logits_pass(info, draft_pair, lm_head, steps)
        inputs_all = spread(jnp.concatenate([by_owner(jnp.concatenate([f_rows, emb_rows], axis=1)), by_owner(hidden0), by_owner(mixed_rows)], axis=2))
        inputs_all = inputs_all.reshape(n * rows, 4 * shard)
        top_t, sum_t = lane_lse(m_t, l_t)
        top_q, sum_q = lane_lse(m_q, l_q)
        mine = jnp.concatenate([top_t, sum_t, top_q, sum_q], axis=1)
        theirs = swap(mine)
        theirs = jnp.concatenate([theirs[rows:], theirs[:rows]], axis=0)

        def merged(k):
            top = jnp.maximum(mine[:, k], theirs[:, k])
            total = mine[:, k + 1] * jnp.exp(mine[:, k] - top) + theirs[:, k + 1] * jnp.exp(theirs[:, k] - top)
            return top + jnp.log(total)

        valid = (lax.rem(lax.broadcasted_iota(jnp.int32, (2 * rows, 1), 0), seq) < seq - 1).astype(F32)

        def lanes(x):
            return jnp.broadcast_to(x.reshape(2 * rows, 1), (2 * rows, 128))

        dy, cross = grad_pass(info, zt, zq, lm_head, lanes(merged(0)), lanes(merged(2)), lanes(valid * (CLS_WEIGHT * inv_count)), steps)
        dy, inputs_all = lax.optimization_barrier((dy, inputs_all))
        dy_own = dy[:rows] + swap(dy[rows:])

        error = (draft_out.astype(F32) - next_rows(f_rows).astype(F32)) * valid[:rows]
        abs_error = jnp.abs(error)
        reg_total = jnp.sum(jnp.where(abs_error < 1.0, 0.5 * error * error, abs_error - 0.5)) / width
        local_loss = reg_total - CLS_WEIGHT * jnp.sum(cross * valid)

        d_out = (jnp.clip(error, -1.0, 1.0) * (inv_count / width) + dy_own) * valid[:rows]
        d_out_all, d_normed, d_gu, sums = exchange(backward_block, 2, d_out.astype(BF16),
                                                   (gu, down, normed_all, h1 * inv_rms, jnp.full((8, 128), local_loss, F32)),
                                                   (n * rows, 2 * wide), 5, True)
        grad_gu = dot(normed_all, d_gu, 0, 0).reshape(n, shard, 2 * wide)
        grad_gu = spread(grad_gu)
        grad_gate = jnp.concatenate([grad_gu[j][:, :ends[j] - starts[j]] for j in range(n)], axis=1)
        grad_up = jnp.concatenate([grad_gu[j][:, wide:wide + ends[j] - starts[j]] for j in range(n)], axis=1)
        grad_down = dot(act, d_out_all, 0, 0)
        edge = 3 * shift
        from_prev = lax.ppermute(grad_down[wide - edge:], AXIS_NAME, [(j, j + 1) for j in range(n - 1) if j % 4 != 3])
        grad_down = lax.dynamic_slice(jnp.concatenate([from_prev, grad_down], axis=0), (edge - shift * place, 0), (hidden // n, width))

        gained = d_normed * gain
        d_hidden1 = d_out + inv_rms * gained - h1 * (inv_rms * inv_rms * inv_rms) * jnp.mean(gained * h1, axis=-1, keepdims=True)
        d_h1 = d_hidden1.astype(BF16)
        total_loss = sums[0, width] * inv_count
        grad_gain = lax.dynamic_slice(sums[0], (me * shard,), (shard,))
        d_h1_all = gather(d_h1)
        d_mixed = dot(d_h1, o_full, 1, 1).astype(BF16)
        d_q, d_k, d_v = attn_vjp(d_mixed.reshape(mixed.shape))
        d_qkv = jnp.concatenate([d_q.reshape(rows, qw).astype(BF16), d_k.reshape(rows, kw).astype(BF16), d_v.reshape(rows, kw)], axis=1)
        d_h0 = (d_hidden1 + dot(d_qkv, qkv_full, 1, 1)).astype(BF16)
        d_qkv_all = gather(d_qkv)
        d_h0_all = gather(d_h0)
        grad_o = dot(inputs_all[:, 3 * shard:], d_h1_all, 0, 0)
        grad_qkv = dot(inputs_all[:, 2 * shard:3 * shard], d_qkv_all, 0, 0)
        grad_fc = dot(inputs_all[:, :2 * shard], d_h0_all, 0, 0)
        grad_bias = jnp.sum(lax.dynamic_slice(d_h0_all, (0, me * shard), (n * rows, shard)).astype(F32), axis=0)
        return (total_loss, grad_fc, grad_bias, grad_qkv[:, :qw].reshape(w_q.shape), grad_qkv[:, qw:qw + kw].reshape(w_k.shape),
                grad_qkv[:, qw + kw:].reshape(w_v.shape), grad_o, grad_gain, grad_gate, grad_up, grad_down)

    return jax.shard_map(local_step, mesh=mesh, in_specs=(split_spec, split_spec, whole_spec, whole_spec) + (split_spec,) * 10,
                         out_specs=(whole_spec,) + (split_spec,) * 10, check_vma=False)
```
